64 devices in a mesh: rep: 4 (over x, y), dp: 16 (over z, core).
Axes of the slice: x: 2, y: 2, z: 8, core: 2. Of those that a mesh axis runs over, the one named last changes fastest.
The devices are a block of a 4x4x8 slice.
Arguments:
- g_w_gate: bfloat16 [64, 2, 1024, 2816], P(('rep', 'dp')), parts along dimension 0
- g_w_up: bfloat16 [64, 2, 1024, 2816], P(('rep', 'dp')), parts along dimension 0
- g_w_down: bfloat16 [64, 2, 2816, 1024], P(('rep', 'dp')), parts along dimension 0
- w_gate: bfloat16 [2, 1024, 2816], replicated
- w_up: bfloat16 [2, 1024, 2816], replicated
- w_down: bfloat16 [2, 2816, 1024], replicated
- m_w_gate: float32 [2, 1024, 2816], P(None, 'dp')
- m_w_up: float32 [2, 1024, 2816], P(None, 'dp')
- m_w_down: float32 [2, 2816, 1024], P(None, 'dp')
- v_w_gate: float32 [2, 1024, 2816], P(None, 'dp')
- v_w_up: float32 [2, 1024, 2816], P(None, 'dp')
- v_w_down: float32 [2, 2816, 1024], P(None, 'dp')
Outputs:
- output 1: bfloat16 [8, 1024, 2816], P('rep'), parts along dimension 0
- output 2: bfloat16 [8, 1024, 2816], P('rep'), parts along dimension 0
- output 3: bfloat16 [8, 2816, 1024], P('rep'), parts along dimension 0
- output 4: float32 [8, 1024, 2816], P('rep', 'dp'), parts along dimension 0
- output 5: float32 [8, 1024, 2816], P('rep', 'dp'), parts along dimension 0
- output 6: float32 [8, 2816, 1024], P('rep', 'dp'), parts along dimension 0
- output 7: float32 [8, 1024, 2816], P('rep', 'dp'), parts along dimension 0
- output 8: float32 [8, 1024, 2816], P('rep', 'dp'), parts along dimension 0
- output 9: float32 [8, 2816, 1024], P('rep', 'dp'), parts along dimension 0
There are 4 independent parts. The reference program is written for one: setup_inputs(seed, part) draws one part's arguments, and reference() takes and returns one part's arrays. A program takes and returns all parts, laid end to end along the dimension named above; an argument that names none is the same for every part.
All inputs are finite; a program needn't handle non-finite values.
Results may differ from the reference program's by a relative error of at most 0.022.
Values are sent between devices in bfloat16 or wider.
A program may use at most 768 MiB of HBM per device.

```python
import jax
import jax.numpy as jnp
from jax import lax

DEVICES = 16
D = 1024
FF = 2816
LAYERS = 2
NAMES = ("w_gate", "w_up", "w_down")
SHAPES = {"w_gate": (LAYERS, D, FF), "w_up": (LAYERS, D, FF), "w_down": (LAYERS, FF, D)}


def setup_inputs(seed: int = 0, part: int = 0) -> dict:
    kz, *keys = jax.random.split(jax.random.key(seed), 1 + 5 * len(NAMES))
    loud = 2.0 ** jax.random.uniform(kz, (), jnp.float32, -1.0, 1.0)
    drawn = {}
    for name, key, both in zip(NAMES, keys[:3], keys[3:6], strict=True):
        own = jax.random.normal(jax.random.fold_in(key, part), (DEVICES, *SHAPES[name]), jnp.float32)
        shared = jax.random.normal(jax.random.fold_in(both, part), SHAPES[name], jnp.float32)
        drawn["g_" + name] = (loud * (0.7 * shared / DEVICES + 0.7 * own * DEVICES**-0.5)).astype(jnp.bfloat16)
    for name, key in zip(NAMES, keys[6:9], strict=True):
        drawn[name] = (jax.random.normal(key, SHAPES[name], jnp.float32) * SHAPES[name][1] ** -0.5).astype(jnp.bfloat16)
    for name, key in zip(NAMES, keys[9:12], strict=True):
        drawn["m_" + name] = loud * 0.5 * jax.random.normal(key, SHAPES[name], jnp.float32)
    for name, key in zip(NAMES, keys[12:15], strict=True):
        drawn["v_" + name] = loud * loud * jax.random.uniform(key, SHAPES[name], jnp.float32, 0.5, 1.5)
    return drawn


def adamw(w, m, v, g):
    m = 0.9 * m + 0.1 * g
    v = 0.95 * v + 0.05 * g * g
    step = m * lax.rsqrt(v + 1e-8) + 0.1 * w
    return (w - 0.02 * step).astype(jnp.bfloat16), m, v


def clipped(gradients, sum_of_squares, count):
    factor = jnp.minimum(1.0, 0.5 * lax.rsqrt(sum_of_squares / count + 1e-30))
    return [g * factor for g in gradients]


def reference(g_w_gate, g_w_up, g_w_down, w_gate, w_up, w_down, m_w_gate, m_w_up, m_w_down, v_w_gate, v_w_up, v_w_down):
    def total(terms):
        return lax.scan(lambda so_far, term: (so_far + term.astype(jnp.float32), None), jnp.zeros(terms.shape[1:], jnp.float32), terms)[0]

    gradients = [total(terms).astype(jnp.bfloat16).astype(jnp.float32) for terms in (g_w_gate, g_w_up, g_w_down)]
    gradients = clipped(gradients, sum(jnp.sum(g * g) for g in gradients), sum(g.size for g in gradients))
    new = [
        adamw(w.astype(jnp.float32), m, v, g)
        for w, m, v, g in zip((w_gate, w_up, w_down), (m_w_gate, m_w_up, m_w_down), (v_w_gate, v_w_up, v_w_down), gradients, strict=True)
    ]
    return tuple(one[which] for which in range(3) for one in new)
```

```python
import functools

import jax
import jax.numpy as jnp
from jax import lax
from jax.experimental import pallas as pl
from jax.experimental.pallas import tpu as pltpu
from jax.sharding import PartitionSpec as P

MESH = pl.DeviceIdType.MESH
CORES = 2
SLAB = 16


def kernel(n, *refs):
    g, w, m_in, v_in = refs[0:3], refs[3:6], refs[6:9], refs[9:12]
    whole, m, v = refs[12:15], refs[15:18], refs[18:21]
    wide_slots, tall_slots, wide_w, tall_w, squares = refs[21:26]
    (load_sem, give_send, give_recv, sum_send, sum_recv, state_sem, norm_send, norm_recv, new_send, new_recv, pass_send, pass_recv) = refs[26:]

    me = lax.axis_index("dp")
    chips = n // CORES
    chip, core = me // CORES, lax.rem(me, CORES)
    partner = {"dp": chip * CORES + (1 - core)}
    ahead = {"dp": lax.rem(chip + 1, chips) * CORES + core}
    behind = {"dp": lax.rem(chip + chips - 1, chips) * CORES + core}
    layers = m[0].shape[0]
    units = [(a, layer) for layer in range(layers) for a in range(3)]
    half = len(units) // 2
    order = [u for pair in zip(range(half), range(half, len(units)), strict=True) for u in pair]
    forward = [u < half for u in range(len(units))]

    def rows(a, block, which):
        size = m[a].shape[1]
        return pl.ds(pl.multiple_of((block * CORES + which) * size, SLAB), size)

    def slot(step, u):
        a, layer = units[u]
        return tall_slots.at[step, layer] if a == 2 else wide_slots.at[step, a * layers + layer]

    def w_own(u):
        a, layer = units[u]
        return tall_w.at[layer] if a == 2 else wide_w.at[a * layers + layer]

    def summed(step, u):
        return lax.rem(chip + 2 * chips - 1 - step, chips) if forward[u] else lax.rem(chip + 1 + step, chips)

    def gathered(step, u):
        return lax.rem(chip + chips - step, chips) if forward[u] else lax.rem(chip + step, chips)

    def remote(src, dst, send, recv, to):
        return pltpu.make_async_remote_copy(src_ref=src, dst_ref=dst, send_sem=send, recv_sem=recv, device_id=to, device_id_type=MESH)

    def load(step, u):
        a, layer = units[u]
        mine = rows(a, summed(step, u), core)
        return pltpu.make_async_copy(g[a].at[0, layer, mine], whole[a].at[layer, mine], load_sem.at[step, u])

    def give(step, u):
        a, layer = units[u]
        block = summed(step, u)
        return remote(
            g[a].at[0, layer, rows(a, block, 1 - core)],
            whole[a].at[layer, rows(a, block, core)],
            give_send.at[step, u],
            give_recv.at[step, u],
            partner,
        )

    def send_sum(step, u):
        a, layer = units[u]
        return remote(
            whole[a].at[layer, rows(a, summed(step, u), core)],
            slot(step, u),
            sum_send.at[step, u],
            sum_recv.at[step, u],
            ahead if forward[u] else behind,
        )

    def send_new(step, u):
        a, layer = units[u]
        mine = whole[a].at[layer, rows(a, gathered(step, u), core)]
        return remote(mine, mine, new_send.at[step, u], new_recv.at[step, u], ahead if forward[u] else behind)

    def pass_new(step, u):
        a, layer = units[u]
        mine = whole[a].at[layer, rows(a, gathered(step, u), core)]
        return remote(mine, mine, pass_send.at[step, u], pass_recv.at[step, u], partner)

    def state(u):
        a, layer = units[u]
        return (
            pltpu.make_async_copy(w[a].at[layer, rows(a, chip, core)], w_own(u), state_sem.at[0, u]),
            pltpu.make_async_copy(m_in[a].at[layer], m[a].at[layer], state_sem.at[1, u]),
            pltpu.make_async_copy(v_in[a].at[layer], v[a].at[layer], state_sem.at[2, u]),
        )

    for u in order:
        load(0, u).start()
    barrier = pltpu.get_barrier_semaphore()
    for other in (partner, ahead, behind):
        pl.semaphore_signal(barrier, inc=1, device_id=other, device_id_type=MESH)
    pl.semaphore_wait(barrier, 3)
    for u in order:
        give(0, u).start()

    def add(step, u, first):
        a, layer = units[u]
        block = summed(step, u)
        size = m[a].shape[1]
        load(step, u).wait()
        give(step, u).wait_recv()
        if not first:
            send_sum(step - 1, u).wait_recv()
        base, other = (block * CORES + core) * size, (block * CORES + 1 - core) * size

        def body(i, squared):
            at = pl.ds(pl.multiple_of(base + i * SLAB, SLAB), SLAB)
            total = whole[a][layer, at, :].astype(jnp.float32)
            total += whole[a][layer, pl.ds(pl.multiple_of(other + i * SLAB, SLAB), SLAB), :].astype(jnp.float32)
            if not first:
                total = slot(step - 1, u)[pl.ds(pl.multiple_of(i * SLAB, SLAB), SLAB), :].astype(jnp.float32) + total
            total = total.astype(jnp.bfloat16)
            whole[a][layer, at, :] = total
            if squared is None:
                return None
            total = total.astype(jnp.float32)
            total = total * total
            pieces = [total[r : r + 8, k : k + 128] for r in range(0, SLAB, 8) for k in range(0, total.shape[1], 128)]
            while len(pieces) > 1:
                pieces = [sum(pieces[k : k + 2]) for k in range(0, len(pieces), 2)]
            return squared + pieces[0]

        return body, size // SLAB

    def add_and_send(step, u, first=False):
        body, count = add(step, u, first)
        lax.fori_loop(0, count, lambda i, _: body(i, None) or 0, 0)
        send_sum(step, u).start()

    def prefetch(step):
        for u in order:
            load(step, u).start()
            give(step, u).start()

    prefetch(1)
    for u in order:
        add_and_send(0, u, first=True)
    for u in order:
        for copy in state(u):
            copy.start()

    def middle(step, carry):
        prefetch(step + 1)
        for u in order:
            add_and_send(step, u)
        return carry

    lax.fori_loop(1, chips - 1, middle, 0)

    total = jnp.zeros((8, 128), jnp.float32)
    for u in order:
        body, count = add(chips - 1, u, False)
        total = lax.fori_loop(0, count, body, total)

    def drained(step, carry):
        for u in order:
            send_sum(step, u).wait_send()
        return carry

    lax.fori_loop(0, chips - 1, drained, 0)

    squares[me] = jnp.sum(total, axis=0, keepdims=True)

    def norm(k):
        return remote(squares.at[me], squares.at[me], norm_send.at[k], norm_recv.at[k], {"dp": lax.rem(me + k, n)})

    for k in range(1, n):
        norm(k).start()
    for u in order:
        for copy in state(u):
            copy.wait()
    for k in range(1, n):
        norm(k).wait_recv()
    every = jnp.sum(jnp.sum(squares[...], axis=0), axis=1, keepdims=True)
    count = n * sum(one.size for one in m)
    factor = jnp.minimum(1.0, 0.5 * lax.rsqrt(every / count + 1e-30))

    for u in order:
        a, layer = units[u]
        base = me * m[a].shape[1]

        def body(i, carry, a=a, layer=layer, u=u, base=base):
            at = pl.ds(pl.multiple_of(i * SLAB, SLAB), SLAB)
            mine = pl.ds(pl.multiple_of(base + i * SLAB, SLAB), SLAB)
            gradient = whole[a][layer, mine, :].astype(jnp.float32) * factor
            weight = w_own(u)[at, :].astype(jnp.float32)
            moment = 0.9 * m[a][layer, at, :] + 0.1 * gradient
            second = 0.95 * v[a][layer, at, :] + 0.05 * gradient * gradient
            m[a][layer, at, :] = moment
            v[a][layer, at, :] = second
            change = moment * lax.rsqrt(second + 1e-8) + 0.1 * weight
            whole[a][layer, mine, :] = (weight - 0.02 * change).astype(jnp.bfloat16)
            return carry

        lax.fori_loop(0, m[a].shape[1] // SLAB, body, 0)
        send_new(0, u).start()
        pass_new(0, u).start()

    def onward(step, carry):
        for u in order:
            send_new(step - 1, u).wait_recv()
            send_new(step, u).start()
            pass_new(step, u).start()
        return carry

    lax.fori_loop(1, chips - 1, onward, 0)
    for u in order:
        send_new(chips - 2, u).wait_recv()
        pass_new(chips - 1, u).start()

    def ended(step, carry):
        for u in order:
            give(step, u).wait_send()
            pass_new(step, u).wait()
        return carry

    lax.fori_loop(0, chips, ended, 0)

    def sent(step, carry):
        for u in order:
            send_new(step, u).wait_send()
        return carry

    lax.fori_loop(0, chips - 1, sent, 0)
    for k in range(1, n):
        norm(k).wait_send()


def write_out(parts, *refs):
    count = (len(refs) - 1) // 2
    copies = []
    for src, dst in zip(refs[:count], refs[count:-1], strict=True):
        layers, size = src.shape[0], src.shape[1] // parts
        for layer in range(layers):
            for part in range(parts):
                at = (layer, pl.ds(part * size, size))
                copies.append(pltpu.make_async_copy(src.at[at], dst.at[at], refs[-1].at[len(copies)]))
    for copy in copies:
        copy.start()
    for copy in copies:
        copy.wait()


def solution(mesh):
    n = mesh.shape["dp"]
    chips = n // CORES

    def step(*arrays):
        weights, m, v = (arrays[i : i + 3] for i in (3, 6, 9))
        layers, wide, columns = m[0].shape
        _, tall, narrow = m[2].shape
        unit = layers * 3
        whole = [pltpu.VMEM(x.shape, x.dtype) for x in weights]
        moments = [pltpu.VMEM(x.shape, x.dtype) for x in (*m, *v)]
        dma = pltpu.SemaphoreType.DMA
        done = pl.pallas_call(
            functools.partial(kernel, n),
            out_shape=[*whole, *moments],
            in_specs=[pl.BlockSpec(memory_space=pltpu.HBM)] * 12,
            out_specs=[pl.BlockSpec(memory_space=pltpu.VMEM)] * 9,
            scratch_shapes=[
                pltpu.VMEM((chips - 1, 2 * layers, wide, columns), jnp.bfloat16),
                pltpu.VMEM((chips - 1, layers, tall, narrow), jnp.bfloat16),
                pltpu.VMEM((2 * layers, wide, columns), jnp.bfloat16),
                pltpu.VMEM((layers, tall, narrow), jnp.bfloat16),
                pltpu.VMEM((n, 1, 128), jnp.float32),
                dma((chips, unit)),
                dma((chips, unit)),
                dma((chips, unit)),
                dma((chips - 1, unit)),
                dma((chips - 1, unit)),
                dma((3, unit)),
                dma((n,)),
                dma((n,)),
                dma((chips - 1, unit)),
                dma((chips - 1, unit)),
                dma((chips, unit)),
                dma((chips, unit)),
            ],
            compiler_params=pltpu.CompilerParams(collective_id=0, has_side_effects=True, vmem_limit_bytes=17 * 2**20),
            name="clipped_step",
        )(*arrays)

        def out(parts, *xs):
            return pl.pallas_call(
                functools.partial(write_out, parts),
                out_shape=[jax.ShapeDtypeStruct(x.shape, x.dtype) for x in xs],
                in_specs=[pl.BlockSpec(memory_space=pltpu.VMEM)] * len(xs),
                out_specs=[pl.BlockSpec(memory_space=pltpu.HBM)] * len(xs),
                scratch_shapes=[dma((len(xs) * layers * parts,))],
                compiler_params=pltpu.CompilerParams(vmem_limit_bytes=2**20),
                name="write_out",
            )(*xs)

        return (*out(4, done[0]), *out(4, done[1]), *out(4, done[2]), *out(1, *done[3:]))

    all_of, cut = P(None, None, None), P(None, "dp", None)
    return jax.shard_map(
        step,
        mesh=mesh,
        in_specs=(P(("rep", "dp"), None, None, None),) * 3 + (all_of,) * 3 + (cut,) * 6,
        out_specs=(P("rep", None, None),) * 3 + (P("rep", "dp", None),) * 6,
        check_vma=False,
    )
```

```python
import functools

import jax
import jax.numpy as jnp
from jax import lax
from jax.experimental import pallas as pl
from jax.experimental.pallas import tpu as pltpu
from jax.sharding import PartitionSpec as P

MESH = pl.DeviceIdType.MESH
CORES = 2
SLAB = 16
TAIL = 48
PIECES = 5
VMEM_LIMIT = 18 * 2**20


def kernel(n, *refs):
    g, w, m_in, v_in = refs[0:3], refs[3:6], refs[6:9], refs[9:12]
    whole, m, v = refs[12:15], refs[15:18], refs[18:21]
    wide_slots, tall_slots, wide_w, tall_w, squares = refs[21:26]
    (load_sem, give_send, give_recv, sum_send, sum_recv, state_sem, norm_send, norm_recv, new_send, new_recv, pass_send, pass_recv) = refs[26:]

    me = lax.axis_index("dp")
    chips = n // CORES
    chip, core = me // CORES, lax.rem(me, CORES)
    partner = {"dp": chip * CORES + (1 - core)}
    ahead = {"dp": lax.rem(chip + 1, chips) * CORES + core}
    behind = {"dp": lax.rem(chip + chips - 1, chips) * CORES + core}
    layers = m[0].shape[0]

    def cut(layer):
        sizes = [x.shape[1] for x in m]
        parts = [(SLAB, sizes[0] - SLAB), (sizes[1],), (sizes[2] - TAIL, TAIL)]
        done = []
        for a, part in enumerate(parts):
            first = 0
            for count in part:
                if count > 0:
                    done.append((a, layer, first, count))
                first += count
        return done

    half = layers // 2
    there = [u for layer in range(half) for u in cut(layer)]
    back = [u for layer in range(half, layers) for u in cut(layer)]
    units = [u for pair in zip(there, back, strict=True) for u in pair]
    order = range(len(units))
    forward = [u % 2 == 0 for u in order]

    def rows(u, block, which):
        a, _, first, count = units[u]
        return pl.ds(pl.multiple_of((block * CORES + which) * m[a].shape[1] + first, SLAB), count)

    def slot(step, u):
        a, layer, first, count = units[u]
        part = pl.ds(first, count)
        return tall_slots.at[step, layer, part] if a == 2 else wide_slots.at[step, a * layers + layer, part]

    def w_own(u):
        a, layer, first, count = units[u]
        part = pl.ds(first, count)
        return tall_w.at[layer, part] if a == 2 else wide_w.at[a * layers + layer, part]

    def summed(step, u):
        return lax.rem(chip + 2 * chips - 1 - step, chips) if forward[u] else lax.rem(chip + 1 + step, chips)

    def gathered(step, u):
        return lax.rem(chip + chips - step, chips) if forward[u] else lax.rem(chip + step, chips)

    def remote(src, dst, send, recv, to):
        return pltpu.make_async_remote_copy(src_ref=src, dst_ref=dst, send_sem=send, recv_sem=recv, device_id=to, device_id_type=MESH)

    def load(step, u):
        a, layer, _, _ = units[u]
        mine = rows(u, summed(step, u), core)
        return pltpu.make_async_copy(g[a].at[0, layer, mine], whole[a].at[layer, mine], load_sem.at[step, u])

    def stage(u):
        a, layer, _, _ = units[u]
        return pltpu.make_async_copy(g[a].at[0, layer, rows(u, summed(0, u), 1 - core)], w_own(u), state_sem.at[0, u])

    def give(step, u, staged=False):
        a, layer, _, _ = units[u]
        block = summed(step, u)
        return remote(
            w_own(u) if staged else g[a].at[0, layer, rows(u, block, 1 - core)],
            whole[a].at[layer, rows(u, block, core)],
            give_send.at[step, u],
            give_recv.at[step, u],
            partner,
        )

    def send_sum(step, u):
        a, layer, _, _ = units[u]
        return remote(
            whole[a].at[layer, rows(u, summed(step, u), core)],
            slot(step, u),
            sum_send.at[step, u],
            sum_recv.at[step, u],
            ahead if forward[u] else behind,
        )

    def send_new(step, u):
        a, layer, _, _ = units[u]
        mine = whole[a].at[layer, rows(u, gathered(step, u), core)]
        return remote(mine, mine, new_send.at[step, u], new_recv.at[step, u], ahead if forward[u] else behind)

    def pass_new(step, u):
        a, layer, _, _ = units[u]
        mine = whole[a].at[layer, rows(u, gathered(step, u), core)]
        return remote(mine, mine, pass_send.at[step, u], pass_recv.at[step, u], partner)

    def state(u):
        a, layer, first, count = units[u]
        part = pl.ds(first, count)
        return (
            pltpu.make_async_copy(w[a].at[layer, rows(u, chip, core)], w_own(u), state_sem.at[0, u]),
            pltpu.make_async_copy(m_in[a].at[layer, part], m[a].at[layer, part], state_sem.at[1, u]),
            pltpu.make_async_copy(v_in[a].at[layer, part], v[a].at[layer, part], state_sem.at[2, u]),
        )

    for u in order:
        stage(u).start()
        load(0, u).start()
    barrier = pltpu.get_barrier_semaphore()
    for other in (partner, ahead, behind):
        pl.semaphore_signal(barrier, inc=1, device_id=other, device_id_type=MESH)
    pl.semaphore_wait(barrier, 3)
    for u in order:
        stage(u).wait()
        give(0, u, staged=True).start()

    def add(step, u, first=False, squared=None):
        a, layer, start, count = units[u]
        size = m[a].shape[1]
        block = summed(step, u)
        load(step, u).wait()
        give(step, u).wait_recv()
        if not first:
            send_sum(step - 1, u).wait_recv()
        mine, other = (block * CORES + core) * size + start, (block * CORES + 1 - core) * size + start

        def body(i, squared):
            at = pl.ds(pl.multiple_of(mine + i * SLAB, SLAB), SLAB)
            total = whole[a][layer, at, :].astype(jnp.float32)
            total += whole[a][layer, pl.ds(pl.multiple_of(other + i * SLAB, SLAB), SLAB), :].astype(jnp.float32)
            if not first:
                total = slot(step - 1, u)[pl.ds(pl.multiple_of(i * SLAB, SLAB), SLAB), :].astype(jnp.float32) + total
            total = total.astype(jnp.bfloat16)
            whole[a][layer, at, :] = total
            if want is None:
                return 0
            total = total.astype(jnp.float32)
            total = total * total
            pieces = [total[r : r + 8, k : k + 128] for r in range(0, SLAB, 8) for k in range(0, total.shape[1], 128)]
            while len(pieces) > 1:
                pieces = [sum(pieces[k : k + 2]) for k in range(0, len(pieces), 2)]
            return squared + pieces[0]

        want = squared
        return lax.fori_loop(0, count // SLAB, body, 0 if want is None else want)

    def add_and_send(step, u, first=False):
        add(step, u, first)
        send_sum(step, u).start()

    def prefetch(step):
        for u in order:
            load(step, u).start()
            give(step, u).start()

    prefetch(1)
    for u in order:
        add_and_send(0, u, first=True)
    for u in order:
        give(0, u, staged=True).wait_send()
        for copy in state(u):
            copy.start()

    def middle(step, carry):
        prefetch(step + 1)
        for u in order:
            add_and_send(step, u)
        for u in order:
            send_sum(step - 1, u).wait_send()
            give(step, u).wait_send()
        return carry

    lax.fori_loop(1, chips - 1, middle, 0)

    total = jnp.zeros((8, 128), jnp.float32)
    for u in order:
        total = add(chips - 1, u, squared=total)
        send_sum(chips - 2, u).wait_send()

    squares[me] = jnp.sum(total, axis=0, keepdims=True)

    def norm(k):
        return remote(squares.at[me], squares.at[me], norm_send.at[k], norm_recv.at[k], {"dp": lax.rem(me + k, n)})

    for k in range(1, n):
        norm(k).start()
    for u in order:
        give(chips - 1, u).wait_send()
        for copy in state(u):
            copy.wait()
    for k in range(1, n):
        norm(k).wait_recv()
    every = jnp.sum(jnp.sum(squares[...], axis=0), axis=1, keepdims=True)
    count = n * sum(one.size for one in m)
    factor = jnp.minimum(1.0, 0.5 * lax.rsqrt(every / count + 1e-30))

    for u in order:
        a, layer, first, count = units[u]
        base = me * m[a].shape[1] + first

        def body(i, carry, a=a, layer=layer, u=u, base=base, first=first):
            at = pl.ds(pl.multiple_of(first + i * SLAB, SLAB), SLAB)
            mine = pl.ds(pl.multiple_of(base + i * SLAB, SLAB), SLAB)
            gradient = whole[a][layer, mine, :].astype(jnp.float32) * factor
            weight = w_own(u)[pl.ds(pl.multiple_of(i * SLAB, SLAB), SLAB), :].astype(jnp.float32)
            moment = 0.9 * m[a][layer, at, :] + 0.1 * gradient
            second = 0.95 * v[a][layer, at, :] + 0.05 * gradient * gradient
            m[a][layer, at, :] = moment
            v[a][layer, at, :] = second
            change = moment * lax.rsqrt(second + 1e-8) + 0.1 * weight
            whole[a][layer, mine, :] = (weight - 0.02 * change).astype(jnp.bfloat16)
            return carry

        lax.fori_loop(0, count // SLAB, body, 0)
        send_new(0, u).start()
        pass_new(0, u).start()

    def onward(step, carry):
        for u in order:
            send_new(step - 1, u).wait_recv()
            send_new(step, u).start()
            pass_new(step, u).start()
        for u in order:
            send_new(step - 1, u).wait_send()
            pass_new(step - 1, u).wait()
        return carry

    lax.fori_loop(1, chips - 1, onward, 0)
    for u in order:
        send_new(chips - 2, u).wait_recv()
        pass_new(chips - 1, u).start()
    for k in range(1, n):
        norm(k).wait_send()
    for u in order:
        send_new(chips - 2, u).wait_send()
        pass_new(chips - 2, u).wait()
    for u in order:
        pass_new(chips - 1, u).wait()


def write_out(*refs):
    count = (len(refs) - 1) // 2
    copies = []
    for src, dst in zip(refs[:count], refs[count:-1], strict=True):
        for layer in range(src.shape[0]):
            copies.append(pltpu.make_async_copy(src.at[layer], dst.at[layer], refs[-1].at[len(copies)]))
    for copy in copies:
        copy.start()
    for copy in copies:
        copy.wait()


def solution(mesh):
    n = mesh.shape["dp"]
    chips = n // CORES

    def step(*arrays):
        weights, m, v = (arrays[i : i + 3] for i in (3, 6, 9))
        layers, wide, columns = m[0].shape
        _, tall, narrow = m[2].shape
        unit = layers * PIECES
        whole = [pltpu.VMEM(x.shape, x.dtype) for x in weights]
        moments = [pltpu.VMEM(x.shape, x.dtype) for x in (*m, *v)]
        dma = pltpu.SemaphoreType.DMA
        done = pl.pallas_call(
            functools.partial(kernel, n),
            out_shape=[*whole, *moments],
            in_specs=[pl.BlockSpec(memory_space=pltpu.HBM)] * 12,
            out_specs=[pl.BlockSpec(memory_space=pltpu.VMEM)] * 9,
            scratch_shapes=[
                pltpu.VMEM((chips - 1, 2 * layers, wide, columns), jnp.bfloat16),
                pltpu.VMEM((chips - 1, layers, tall, narrow), jnp.bfloat16),
                pltpu.VMEM((2 * layers, wide, columns), jnp.bfloat16),
                pltpu.VMEM((layers, tall, narrow), jnp.bfloat16),
                pltpu.VMEM((n, 1, 128), jnp.float32),
                dma((chips, unit)),
                dma((chips, unit)),
                dma((chips, unit)),
                dma((chips - 1, unit)),
                dma((chips - 1, unit)),
                dma((3, unit)),
                dma((n,)),
                dma((n,)),
                dma((chips - 1, unit)),
                dma((chips - 1, unit)),
                dma((chips, unit)),
                dma((chips, unit)),
            ],
            compiler_params=pltpu.CompilerParams(collective_id=0, has_side_effects=True, vmem_limit_bytes=VMEM_LIMIT),
            name="clipped_step",
        )(*arrays)

        def out(*xs):
            return pl.pallas_call(
                write_out,
                out_shape=[jax.ShapeDtypeStruct(x.shape, x.dtype) for x in xs],
                in_specs=[pl.BlockSpec(memory_space=pltpu.VMEM)] * len(xs),
                out_specs=[pl.BlockSpec(memory_space=pltpu.HBM)] * len(xs),
                scratch_shapes=[dma((len(xs) * layers,))],
                compiler_params=pltpu.CompilerParams(vmem_limit_bytes=VMEM_LIMIT),
                name="write_out",
            )(*xs)

        moments = out(*done[3:])
        return (*out(*done[:3]), *moments)

    all_of, cut = P(None, None, None), P(None, "dp", None)
    return jax.shard_map(
        step,
        mesh=mesh,
        in_specs=(P(("rep", "dp"), None, None, None),) * 3 + (all_of,) * 3 + (cut,) * 6,
        out_specs=(P("rep", None, None),) * 3 + (P("rep", "dp", None),) * 6,
        check_vma=False,
    )
```

```python
import functools

import jax
import jax.numpy as jnp
from jax import lax
from jax.experimental import pallas as pl
from jax.experimental.pallas import tpu as pltpu
from jax.sharding import PartitionSpec as P

MESH = pl.DeviceIdType.MESH
CORES = 2
SLAB = 16
TAIL = 48
PIECES = 5
VMEM_LIMIT = 18 * 2**20


def kernel(n, *refs):
    g, w, m_in, v_in = refs[0:3], refs[3:6], refs[6:9], refs[9:12]
    whole, m, v = refs[12:15], refs[15:18], refs[18:21]
    wide_slots, tall_slots, wide_w, tall_w, squares = refs[21:26]
    load_sem, across_send, across_recv, ring_send, ring_recv, w_sem, moment_sem, norm_send, norm_recv = refs[26:]

    me = lax.axis_index("dp")
    chips = n // CORES
    chip, core = me // CORES, lax.rem(me, CORES)
    partner = {"dp": chip * CORES + (1 - core)}
    ahead = {"dp": lax.rem(chip + 1, chips) * CORES + core}
    behind = {"dp": lax.rem(chip + chips - 1, chips) * CORES + core}
    layers = m[0].shape[0]

    def cut(layer):
        sizes = [x.shape[1] for x in m]
        parts = [(SLAB, sizes[0] - SLAB), (sizes[1],), (sizes[2] - TAIL, TAIL)]
        done = []
        for a, part in enumerate(parts):
            first = 0
            for count in part:
                if count > 0:
                    done.append((a, layer, first, count))
                first += count
        return done

    half = layers // 2
    there = [u for layer in range(half) for u in cut(layer)]
    back = [u for layer in range(half, layers) for u in cut(layer)]
    units = [u for pair in zip(there, back, strict=True) for u in pair]
    order = range(len(units))
    forward = [u % 2 == 0 for u in order]

    def rows(u, block, which):
        a, _, first, count = units[u]
        return pl.ds(pl.multiple_of((block * CORES + which) * m[a].shape[1] + first, SLAB), count)

    def slot(step, u):
        a, layer, first, count = units[u]
        part = pl.ds(first, count)
        return tall_slots.at[step, layer, part] if a == 2 else wide_slots.at[step, a * layers + layer, part]

    def w_own(u):
        a, layer, first, count = units[u]
        part = pl.ds(first, count)
        return tall_w.at[layer, part] if a == 2 else wide_w.at[a * layers + layer, part]

    def summed(step, u):
        return lax.rem(chip + 2 * chips - 1 - step, chips) if forward[u] else lax.rem(chip + 1 + step, chips)

    def gathered(step, u):
        return lax.rem(chip + chips - step, chips) if forward[u] else lax.rem(chip + step, chips)

    def remote(src, dst, send, recv, to):
        return pltpu.make_async_remote_copy(src_ref=src, dst_ref=dst, send_sem=send, recv_sem=recv, device_id=to, device_id_type=MESH)

    def turn(step):
        return step % 2 if isinstance(step, int) else lax.rem(step, 2)

    def load(step, u):
        a, layer, _, _ = units[u]
        mine = rows(u, summed(step, u), core)
        return pltpu.make_async_copy(g[a].at[0, layer, mine], whole[a].at[layer, mine], load_sem.at[turn(step), u])

    def stage(u):
        a, layer, _, _ = units[u]
        return pltpu.make_async_copy(g[a].at[0, layer, rows(u, summed(0, u), 1 - core)], w_own(u), load_sem.at[1, u])

    def give(step, u, staged=False):
        a, layer, _, _ = units[u]
        block = summed(step, u)
        return remote(
            w_own(u) if staged else g[a].at[0, layer, rows(u, block, 1 - core)],
            whole[a].at[layer, rows(u, block, core)],
            across_send.at[turn(step), u],
            across_recv.at[step, u],
            partner,
        )

    def send_sum(step, u):
        a, layer, _, _ = units[u]
        return remote(
            whole[a].at[layer, rows(u, summed(step, u), core)],
            slot(step, u),
            ring_send.at[turn(step), u],
            ring_recv.at[step, u],
            ahead if forward[u] else behind,
        )

    def send_new(step, u):
        a, layer, _, _ = units[u]
        mine = whole[a].at[layer, rows(u, gathered(step, u), core)]
        return remote(mine, mine, ring_send.at[turn(step), u], ring_recv.at[step, u], ahead if forward[u] else behind)

    def pass_new(step, u):
        a, layer, _, _ = units[u]
        mine = whole[a].at[layer, rows(u, gathered(step, u), core)]
        return remote(mine, mine, across_send.at[turn(step), u], across_recv.at[step, u], partner)

    def own_weights(u):
        a, layer, _, _ = units[u]
        return pltpu.make_async_copy(w[a].at[layer, rows(u, chip, core)], w_own(u), w_sem.at[u])

    def moments(a):
        return (
            pltpu.make_async_copy(m_in[a], m[a], moment_sem.at[0, a]),
            pltpu.make_async_copy(v_in[a], v[a], moment_sem.at[1, a]),
        )

    def fetch(u):
        stage(u).start()
        load(0, u).start()

    first_of_each, rest = order[:2], order[2:]
    for u in first_of_each:
        fetch(u)
    barrier = pltpu.get_barrier_semaphore()
    for other in (partner, ahead, behind):
        pl.semaphore_signal(barrier, inc=1, device_id=other, device_id_type=MESH)
    for u in rest:
        fetch(u)
    for u in first_of_each:
        stage(u).wait()
    pl.semaphore_wait(barrier, 3)
    for u in first_of_each:
        give(0, u, staged=True).start()
    for u in rest:
        stage(u).wait()
        give(0, u, staged=True).start()

    def add(step, u, first=False, squared=None):
        a, layer, start, count = units[u]
        size = m[a].shape[1]
        block = summed(step, u)
        load(step, u).wait()
        give(step, u).wait_recv()
        if not first:
            send_sum(step - 1, u).wait_recv()
        mine, other = (block * CORES + core) * size + start, (block * CORES + 1 - core) * size + start

        def body(i, squared):
            at = pl.ds(pl.multiple_of(mine + i * SLAB, SLAB), SLAB)
            total = whole[a][layer, at, :].astype(jnp.float32)
            total += whole[a][layer, pl.ds(pl.multiple_of(other + i * SLAB, SLAB), SLAB), :].astype(jnp.float32)
            if not first:
                total = slot(step - 1, u)[pl.ds(pl.multiple_of(i * SLAB, SLAB), SLAB), :].astype(jnp.float32) + total
            total = total.astype(jnp.bfloat16)
            whole[a][layer, at, :] = total
            if want is None:
                return 0
            total = total.astype(jnp.float32)
            total = total * total
            pieces = [total[r : r + 8, k : k + 128] for r in range(0, SLAB, 8) for k in range(0, total.shape[1], 128)]
            while len(pieces) > 1:
                pieces = [sum(pieces[k : k + 2]) for k in range(0, len(pieces), 2)]
            return squared + pieces[0]

        want = squared
        return lax.fori_loop(0, count // SLAB, body, 0 if want is None else want)

    def fetch_next(step):
        for u in order:
            load(step + 1, u).start()
            if not isinstance(step, int) or step > 0:
                give(step - 1, u).wait_send()
            give(step + 1, u).start()

    for u in order:
        add(0, u, first=True)
        send_sum(0, u).start()
    fetch_next(0)
    fetch_next(1)
    for u in order:
        add(1, u)
        send_sum(1, u).start()
    for u in order:
        own_weights(u).start()
    for a in range(3):
        for copy in moments(a):
            copy.start()

    def middle(step, carry):
        fetch_next(step)
        for u in order:
            add(step, u)
            send_sum(step - 2, u).wait_send()
            send_sum(step, u).start()
        return carry

    lax.fori_loop(2, chips - 1, middle, 0)

    total = jnp.zeros((8, 128), jnp.float32)
    for u in order:
        total = add(chips - 1, u, squared=total)
    for u in order:
        send_sum(chips - 3, u).wait_send()
        send_sum(chips - 2, u).wait_send()

    squares[me] = jnp.sum(total, axis=0, keepdims=True)

    def norm(k):
        return remote(squares.at[me], squares.at[me], norm_send.at[k], norm_recv.at[k], {"dp": lax.rem(me + k, n)})

    for k in sorted(range(1, n), key=lambda k: abs(k - n // 2)):
        norm(k).start()
    for u in order:
        give(chips - 2, u).wait_send()
        give(chips - 1, u).wait_send()
        own_weights(u).wait()
    for a in range(3):
        for copy in moments(a):
            copy.wait()
    for k in range(1, n):
        norm(k).wait_recv()
    every = jnp.sum(jnp.sum(squares[...], axis=0), axis=1, keepdims=True)
    count = n * sum(one.size for one in m)
    factor = jnp.minimum(1.0, 0.5 * lax.rsqrt(every / count + 1e-30))

    for u in order:
        a, layer, first, count = units[u]
        base = me * m[a].shape[1] + first

        def body(i, carry, a=a, layer=layer, u=u, base=base, first=first):
            at = pl.ds(pl.multiple_of(first + i * SLAB, SLAB), SLAB)
            mine = pl.ds(pl.multiple_of(base + i * SLAB, SLAB), SLAB)
            gradient = whole[a][layer, mine, :].astype(jnp.float32) * factor
            weight = w_own(u)[pl.ds(pl.multiple_of(i * SLAB, SLAB), SLAB), :].astype(jnp.float32)
            moment = 0.9 * m[a][layer, at, :] + 0.1 * gradient
            second = 0.95 * v[a][layer, at, :] + 0.05 * gradient * gradient
            m[a][layer, at, :] = moment
            v[a][layer, at, :] = second
            change = moment * lax.rsqrt(second + 1e-8) + 0.1 * weight
            whole[a][layer, mine, :] = (weight - 0.02 * change).astype(jnp.bfloat16)
            return carry

        lax.fori_loop(0, count // SLAB, body, 0)
        send_new(0, u).start()
        pass_new(0, u).start()

    def onward(step, u):
        send_new(step - 1, u).wait_recv()
        if not isinstance(step, int) or step > 1:
            send_new(step - 2, u).wait_send()
            pass_new(step - 2, u).wait()
        send_new(step, u).start()
        pass_new(step, u).start()

    for u in order:
        onward(1, u)

    def later(step, carry):
        for u in order:
            onward(step, u)
        return carry

    lax.fori_loop(2, chips - 1, later, 0)
    for u in order:
        send_new(chips - 2, u).wait_recv()
        pass_new(chips - 3, u).wait()
        pass_new(chips - 1, u).start()
    for k in range(1, n):
        norm(k).wait_send()
    for u in order:
        send_new(chips - 3, u).wait_send()
        send_new(chips - 2, u).wait_send()
        pass_new(chips - 2, u).wait()
    for u in order:
        pass_new(chips - 1, u).wait()


def write_out(*refs):
    count = (len(refs) - 1) // 2
    copies = []
    for src, dst in zip(refs[:count], refs[count:-1], strict=True):
        for layer in range(src.shape[0]):
            copies.append(pltpu.make_async_copy(src.at[layer], dst.at[layer], refs[-1].at[len(copies)]))
    for copy in copies:
        copy.start()
    for copy in copies:
        copy.wait()


def solution(mesh):
    n = mesh.shape["dp"]
    chips = n // CORES

    def step(*arrays):
        weights, m, v = (arrays[i : i + 3] for i in (3, 6, 9))
        layers, wide, columns = m[0].shape
        _, tall, narrow = m[2].shape
        unit = layers * PIECES
        whole = [pltpu.VMEM(x.shape, x.dtype) for x in weights]
        states = [pltpu.VMEM(x.shape, x.dtype) for x in (*m, *v)]
        dma = pltpu.SemaphoreType.DMA
        done = pl.pallas_call(
            functools.partial(kernel, n),
            out_shape=[*whole, *states],
            in_specs=[pl.BlockSpec(memory_space=pltpu.HBM)] * 12,
            out_specs=[pl.BlockSpec(memory_space=pltpu.VMEM)] * 9,
            scratch_shapes=[
                pltpu.VMEM((chips - 1, 2 * layers, wide, columns), jnp.bfloat16),
                pltpu.VMEM((chips - 1, layers, tall, narrow), jnp.bfloat16),
                pltpu.VMEM((2 * layers, wide, columns), jnp.bfloat16),
                pltpu.VMEM((layers, tall, narrow), jnp.bfloat16),
                pltpu.VMEM((n, 1, 128), jnp.float32),
                dma((2, unit)),
                dma((2, unit)),
                dma((chips, unit)),
                dma((2, unit)),
                dma((chips - 1, unit)),
                dma((unit,)),
                dma((2, 3)),
                dma((n,)),
                dma((n,)),
            ],
            compiler_params=pltpu.CompilerParams(collective_id=0, has_side_effects=True, vmem_limit_bytes=VMEM_LIMIT),
            name="clipped_step",
        )(*arrays)

        def out(*xs):
            return pl.pallas_call(
                write_out,
                out_shape=[jax.ShapeDtypeStruct(x.shape, x.dtype) for x in xs],
                in_specs=[pl.BlockSpec(memory_space=pltpu.VMEM)] * len(xs),
                out_specs=[pl.BlockSpec(memory_space=pltpu.HBM)] * len(xs),
                scratch_shapes=[dma((len(xs) * layers,))],
                compiler_params=pltpu.CompilerParams(vmem_limit_bytes=VMEM_LIMIT),
                name="write_out",
            )(*xs)

        return (*out(*done[:3]), *out(*done[3:]))

    all_of, cut = P(None, None, None), P(None, "dp", None)
    return jax.shard_map(
        step,
        mesh=mesh,
        in_specs=(P(("rep", "dp"), None, None, None),) * 3 + (all_of,) * 3 + (cut,) * 6,
        out_specs=(P("rep", None, None),) * 3 + (P("rep", "dp", None),) * 6,
        check_vma=False,
    )
```

```python
import functools

import jax
import jax.numpy as jnp
from jax import lax
from jax.experimental import pallas as pl
from jax.experimental.pallas import tpu as pltpu
from jax.sharding import PartitionSpec as P

MESH = pl.DeviceIdType.MESH
CORES = 2
SLAB = 16
TAIL = 48
PIECES = 5
PARTS = 4
VMEM_LIMIT = 18 * 2**20


def kernel(n, *refs):
    g, w, m_in, v_in = refs[0:3], refs[3:6], refs[6:9], refs[9:12]
    whole, m, v = refs[12:15], refs[15:18], refs[18:21]
    wide_slots, tall_slots, wide_w, tall_w, squares = refs[21:26]
    load_sem, across_send, across_recv, ring_send, ring_recv, moment_sem, norm_send, norm_recv = refs[26:]

    me = lax.axis_index("dp")
    chips = n // CORES
    chip, core = me // CORES, lax.rem(me, CORES)
    partner = {"dp": chip * CORES + (1 - core)}
    ahead = {"dp": lax.rem(chip + 1, chips) * CORES + core}
    behind = {"dp": lax.rem(chip + chips - 1, chips) * CORES + core}
    layers = m[0].shape[0]

    def cut(layer):
        sizes = [x.shape[1] for x in m]
        parts = [(SLAB, sizes[0] - SLAB), (sizes[1],), (sizes[2] - TAIL, TAIL)]
        done = []
        for a, part in enumerate(parts):
            first = 0
            for count in part:
                if count > 0:
                    done.append((a, layer, first, count))
                first += count
        return done

    half = layers // 2
    there = [u for layer in range(half) for u in cut(layer)]
    back = [u for layer in range(half, layers) for u in cut(layer)]
    units = [u for pair in zip(there, back, strict=True) for u in pair]
    order = range(len(units))
    forward = [u % 2 == 0 for u in order]

    def rows(u, block, which):
        a, _, first, count = units[u]
        return pl.ds(pl.multiple_of((block * CORES + which) * m[a].shape[1] + first, SLAB), count)

    def slot(step, u):
        a, layer, first, count = units[u]
        part = pl.ds(first, count)
        return tall_slots.at[step, layer, part] if a == 2 else wide_slots.at[step, a * layers + layer, part]

    def w_own(u):
        a, layer, first, count = units[u]
        part = pl.ds(first, count)
        return tall_w.at[layer, part] if a == 2 else wide_w.at[a * layers + layer, part]

    def summed(step, u):
        return lax.rem(chip + 2 * chips - 1 - step, chips) if forward[u] else lax.rem(chip + 1 + step, chips)

    def gathered(step, u):
        return lax.rem(chip + chips - step, chips) if forward[u] else lax.rem(chip + step, chips)

    def remote(src, dst, send, recv, to):
        return pltpu.make_async_remote_copy(src_ref=src, dst_ref=dst, send_sem=send, recv_sem=recv, device_id=to, device_id_type=MESH)

    def turn(step):
        return step % 2 if isinstance(step, int) else lax.rem(step, 2)

    def load(step, u):
        a, layer, _, _ = units[u]
        mine = rows(u, summed(step, u), core)
        return pltpu.make_async_copy(g[a].at[0, layer, mine], whole[a].at[layer, mine], load_sem.at[turn(step), u])

    def stage(u):
        a, layer, _, _ = units[u]
        return pltpu.make_async_copy(g[a].at[0, layer, rows(u, summed(0, u), 1 - core)], w_own(u), load_sem.at[1, u])

    def give(step, u, staged=False):
        a, layer, _, _ = units[u]
        block = summed(step, u)
        return remote(
            w_own(u) if staged else g[a].at[0, layer, rows(u, block, 1 - core)],
            whole[a].at[layer, rows(u, block, core)],
            across_send.at[u],
            across_recv.at[step, u],
            partner,
        )

    def send_sum(step, u):
        a, layer, _, _ = units[u]
        return remote(
            whole[a].at[layer, rows(u, summed(step, u), core)],
            slot(step, u),
            ring_send.at[u],
            ring_recv.at[step, u],
            ahead if forward[u] else behind,
        )

    def send_new(step, u):
        a, layer, _, _ = units[u]
        mine = whole[a].at[layer, rows(u, gathered(step, u), core)]
        return remote(mine, mine, ring_send.at[u], ring_recv.at[step, u], ahead if forward[u] else behind)

    def pass_new(step, u):
        a, layer, _, _ = units[u]
        mine = whole[a].at[layer, rows(u, gathered(step, u), core)]
        return remote(mine, mine, across_send.at[u], across_recv.at[step, u], partner)

    def own_weights(u):
        a, layer, _, _ = units[u]
        return pltpu.make_async_copy(w[a].at[layer, rows(u, chip, core)], w_own(u), load_sem.at[turn(chips), u])

    def moments(a):
        return (
            pltpu.make_async_copy(m_in[a], m[a], moment_sem.at[0, a]),
            pltpu.make_async_copy(v_in[a], v[a], moment_sem.at[1, a]),
        )

    def fetch(u):
        stage(u).start()
        load(0, u).start()

    first_of_each, rest = order[:2], order[2:]
    for u in first_of_each:
        fetch(u)
    barrier = pltpu.get_barrier_semaphore()
    for other in (partner, ahead, behind):
        pl.semaphore_signal(barrier, inc=1, device_id=other, device_id_type=MESH)
    for u in rest:
        fetch(u)
    for u in first_of_each:
        stage(u).wait()
    pl.semaphore_wait(barrier, 3)
    for u in first_of_each:
        give(0, u, staged=True).start()
    for u in rest:
        stage(u).wait()
        give(0, u, staged=True).start()

    def add(step, u, first=False, squared=None):
        a, layer, start, count = units[u]
        size = m[a].shape[1]
        block = summed(step, u)
        load(step, u).wait()
        give(step, u).wait_recv()
        if not first:
            send_sum(step - 1, u).wait_recv()
        mine, other = (block * CORES + core) * size + start, (block * CORES + 1 - core) * size + start

        def body(i, squared):
            at = pl.ds(pl.multiple_of(mine + i * SLAB, SLAB), SLAB)
            total = whole[a][layer, at, :].astype(jnp.float32)
            total += whole[a][layer, pl.ds(pl.multiple_of(other + i * SLAB, SLAB), SLAB), :].astype(jnp.float32)
            if not first:
                total = slot(step - 1, u)[pl.ds(pl.multiple_of(i * SLAB, SLAB), SLAB), :].astype(jnp.float32) + total
            total = total.astype(jnp.bfloat16)
            whole[a][layer, at, :] = total
            if want is None:
                return 0
            total = total.astype(jnp.float32)
            total = total * total
            pieces = [total[r : r + 8, k : k + 128] for r in range(0, SLAB, 8) for k in range(0, total.shape[1], 128)]
            while len(pieces) > 1:
                pieces = [sum(pieces[k : k + 2]) for k in range(0, len(pieces), 2)]
            return squared + pieces[0]

        want = squared
        return lax.fori_loop(0, count // SLAB, body, 0 if want is None else want)

    def fetch_next(step):
        for u in order:
            load(step + 1, u).start()
            give(step, u).wait_send()
            give(step + 1, u).start()

    for u in order:
        add(0, u, first=True)
        send_sum(0, u).start()
    fetch_next(0)
    for a in range(3):
        for copy in moments(a):
            copy.start()

    def middle(step, carry):
        fetch_next(step)
        for u in order:
            add(step, u)
            send_sum(step - 1, u).wait_send()
            send_sum(step, u).start()
        return carry

    lax.fori_loop(1, chips - 1, middle, 0)
    for u in order:
        own_weights(u).start()

    total = jnp.zeros((8, 128), jnp.float32)
    for u in order:
        total = add(chips - 1, u, squared=total)
    for u in order:
        send_sum(chips - 2, u).wait_send()

    squares[me] = jnp.sum(total, axis=0, keepdims=True)

    def norm(k):
        return remote(squares.at[me], squares.at[me], norm_send.at[k], norm_recv.at[k], {"dp": lax.rem(me + k, n)})

    for k in sorted(range(1, n), key=lambda k: abs(k - n // 2)):
        norm(k).start()
    for u in order:
        give(chips - 1, u).wait_send()
        own_weights(u).wait()
    for a in range(3):
        for copy in moments(a):
            copy.wait()
    for k in range(1, n):
        norm(k).wait_recv()
    every = jnp.sum(jnp.sum(squares[...], axis=0), axis=1, keepdims=True)
    count = n * sum(one.size for one in m)
    factor = jnp.minimum(1.0, 0.5 * lax.rsqrt(every / count + 1e-30))

    for u in order:
        a, layer, first, count = units[u]
        base = me * m[a].shape[1] + first

        def body(i, carry, a=a, layer=layer, u=u, base=base, first=first):
            at = pl.ds(pl.multiple_of(first + i * SLAB, SLAB), SLAB)
            mine = pl.ds(pl.multiple_of(base + i * SLAB, SLAB), SLAB)
            gradient = whole[a][layer, mine, :].astype(jnp.float32) * factor
            weight = w_own(u)[pl.ds(pl.multiple_of(i * SLAB, SLAB), SLAB), :].astype(jnp.float32)
            moment = 0.9 * m[a][layer, at, :] + 0.1 * gradient
            second = 0.95 * v[a][layer, at, :] + 0.05 * gradient * gradient
            m[a][layer, at, :] = moment
            v[a][layer, at, :] = second
            change = moment * lax.rsqrt(second + 1e-8) + 0.1 * weight
            whole[a][layer, mine, :] = (weight - 0.02 * change).astype(jnp.bfloat16)
            return carry

        lax.fori_loop(0, count // SLAB, body, 0)
        send_new(0, u).start()
        pass_new(0, u).start()

    def onward(step, u):
        send_new(step - 1, u).wait()
        pass_new(step - 1, u).wait_send()
        send_new(step, u).start()
        pass_new(step, u).start()

    def later(step, carry):
        for u in order:
            onward(step, u)
        for u in order:
            pass_new(step - 1, u).wait_recv()
        return carry

    lax.fori_loop(1, chips - 1, later, 0)
    for u in order:
        send_new(chips - 2, u).wait()
        pass_new(chips - 2, u).wait_send()
        pass_new(chips - 1, u).start()
    for k in range(1, n):
        norm(k).wait_send()
    for u in order:
        pass_new(chips - 2, u).wait_recv()
    for u in order:
        pass_new(chips - 1, u).wait()


def write_out(*refs):
    count = (len(refs) - 1) // 2
    copies = []
    for src, dst in zip(refs[:count], refs[count:-1], strict=True):
        parts = PARTS if src.dtype == jnp.bfloat16 else 1
        size = src.shape[1] // parts
        for layer in range(src.shape[0]):
            for part in range(parts):
                at = layer, pl.ds(part * size, size)
                copies.append(pltpu.make_async_copy(src.at[at], dst.at[at], refs[-1].at[len(copies)]))
    for copy in copies:
        copy.start()
    for copy in copies:
        copy.wait()


def solution(mesh):
    n = mesh.shape["dp"]
    chips = n // CORES

    def step(*arrays):
        weights, m, v = (arrays[i : i + 3] for i in (3, 6, 9))
        layers, wide, columns = m[0].shape
        _, tall, narrow = m[2].shape
        unit = layers * PIECES
        whole = [pltpu.VMEM(x.shape, x.dtype) for x in weights]
        states = [pltpu.VMEM(x.shape, x.dtype) for x in (*m, *v)]
        dma = pltpu.SemaphoreType.DMA
        done = pl.pallas_call(
            functools.partial(kernel, n),
            out_shape=[*whole, *states],
            in_specs=[pl.BlockSpec(memory_space=pltpu.HBM)] * 12,
            out_specs=[pl.BlockSpec(memory_space=pltpu.VMEM)] * 9,
            scratch_shapes=[
                pltpu.VMEM((chips - 1, 2 * layers, wide, columns), jnp.bfloat16),
                pltpu.VMEM((chips - 1, layers, tall, narrow), jnp.bfloat16),
                pltpu.VMEM((2 * layers, wide, columns), jnp.bfloat16),
                pltpu.VMEM((layers, tall, narrow), jnp.bfloat16),
                pltpu.VMEM((n, 1, 128), jnp.float32),
                dma((2, unit)),
                dma((unit,)),
                dma((chips, unit)),
                dma((unit,)),
                dma((chips - 1, unit)),
                dma((2, 3)),
                dma((n,)),
                dma((n,)),
            ],
            compiler_params=pltpu.CompilerParams(collective_id=0, has_side_effects=True, vmem_limit_bytes=VMEM_LIMIT),
            name="clipped_step",
        )(*arrays)

        def out(*xs):
            return pl.pallas_call(
                write_out,
                out_shape=[jax.ShapeDtypeStruct(x.shape, x.dtype) for x in xs],
                in_specs=[pl.BlockSpec(memory_space=pltpu.VMEM)] * len(xs),
                out_specs=[pl.BlockSpec(memory_space=pltpu.HBM)] * len(xs),
                scratch_shapes=[dma((sum(layers * (PARTS if x.dtype == jnp.bfloat16 else 1) for x in xs),))],
                compiler_params=pltpu.CompilerParams(vmem_limit_bytes=VMEM_LIMIT),
                name="write_out",
            )(*xs)

        return (*out(*done[:3]), *out(*done[3:]))

    all_of, cut = P(None, None, None), P(None, "dp", None)
    return jax.shard_map(
        step,
        mesh=mesh,
        in_specs=(P(("rep", "dp"), None, None, None),) * 3 + (all_of,) * 3 + (cut,) * 6,
        out_specs=(P("rep", None, None),) * 3 + (P("rep", "dp", None),) * 6,
        check_vma=False,
    )
```

```python
import functools

import jax
import jax.numpy as jnp
from jax import lax
from jax.experimental import pallas as pl
from jax.experimental.pallas import tpu as pltpu
from jax.sharding import PartitionSpec as P

MESH = pl.DeviceIdType.MESH
CORES = 2
SLAB = 16
TAIL = 48
PIECES = 5
PARTS = 4
VMEM_LIMIT = 18 * 2**20


def kernel(n, *refs):
    g, w, m_in, v_in = refs[0:3], refs[3:6], refs[6:9], refs[9:12]
    whole, m, v = refs[12:15], refs[15:18], refs[18:21]
    wide_slots, tall_slots, wide_w, tall_w, squares = refs[21:26]
    load_sem, across_send, across_recv, ring_send, ring_recv, moment_sem, norm_recv = refs[26:]

    me = lax.axis_index("dp")
    chips = n // CORES
    chip, core = me // CORES, lax.rem(me, CORES)
    partner = {"dp": chip * CORES + (1 - core)}
    ahead = {"dp": lax.rem(chip + 1, chips) * CORES + core}
    behind = {"dp": lax.rem(chip + chips - 1, chips) * CORES + core}
    layers = m[0].shape[0]

    def cut(layer):
        sizes = [x.shape[1] for x in m]
        parts = [(SLAB, sizes[0] - SLAB), (sizes[1],), (sizes[2] - TAIL, TAIL)]
        done = []
        for a, part in enumerate(parts):
            first = 0
            for count in part:
                if count > 0:
                    done.append((a, layer, first, count))
                first += count
        return done

    half = layers // 2
    there = [u for layer in range(half) for u in cut(layer)]
    back = [u for layer in range(half, layers) for u in cut(layer)]
    units = [u for pair in zip(there, back, strict=True) for u in pair]
    order = range(len(units))
    forward = [u % 2 == 0 for u in order]

    def rows(u, block, which):
        a, _, first, count = units[u]
        return pl.ds(pl.multiple_of((block * CORES + which) * m[a].shape[1] + first, SLAB), count)

    def slot(step, u):
        a, layer, first, count = units[u]
        part = pl.ds(first, count)
        return tall_slots.at[step, layer, part] if a == 2 else wide_slots.at[step, a * layers + layer, part]

    def w_own(u):
        a, layer, first, count = units[u]
        part = pl.ds(first, count)
        return tall_w.at[layer, part] if a == 2 else wide_w.at[a * layers + layer, part]

    def summed(step, u):
        return lax.rem(chip + 2 * chips - 1 - step, chips) if forward[u] else lax.rem(chip + 1 + step, chips)

    def gathered(step, u):
        return lax.rem(chip + chips - step, chips) if forward[u] else lax.rem(chip + step, chips)

    def remote(src, dst, send, recv, to):
        return pltpu.make_async_remote_copy(src_ref=src, dst_ref=dst, send_sem=send, recv_sem=recv, device_id=to, device_id_type=MESH)

    def turn(step):
        return step % 2 if isinstance(step, int) else lax.rem(step, 2)

    def load(step, u):
        a, layer, _, _ = units[u]
        mine = rows(u, summed(step, u), core)
        return pltpu.make_async_copy(g[a].at[0, layer, mine], whole[a].at[layer, mine], load_sem.at[turn(step), u])

    def stage(u):
        a, layer, _, _ = units[u]
        return pltpu.make_async_copy(g[a].at[0, layer, rows(u, summed(0, u), 1 - core)], w_own(u), load_sem.at[1, u])

    def give(step, u, staged=False):
        a, layer, _, _ = units[u]
        block = summed(step, u)
        return remote(
            w_own(u) if staged else g[a].at[0, layer, rows(u, block, 1 - core)],
            whole[a].at[layer, rows(u, block, core)],
            across_send.at[u],
            across_recv.at[step, u],
            partner,
        )

    def send_sum(step, u):
        a, layer, _, _ = units[u]
        return remote(
            whole[a].at[layer, rows(u, summed(step, u), core)],
            slot(step, u),
            ring_send.at[u],
            ring_recv.at[step, u],
            ahead if forward[u] else behind,
        )

    def send_new(step, u):
        a, layer, _, _ = units[u]
        mine = whole[a].at[layer, rows(u, gathered(step, u), core)]
        return remote(mine, mine, ring_send.at[u], ring_recv.at[step, u], ahead if forward[u] else behind)

    def pass_new(step, u):
        a, layer, _, _ = units[u]
        mine = whole[a].at[layer, rows(u, gathered(step, u), core)]
        return remote(mine, mine, across_send.at[u], across_recv.at[step, u], partner)

    def own_weights(u):
        a, layer, _, _ = units[u]
        return pltpu.make_async_copy(w[a].at[layer, rows(u, chip, core)], w_own(u), load_sem.at[turn(chips), u])

    def moments(a):
        return (
            pltpu.make_async_copy(m_in[a], m[a], moment_sem.at[0, a]),
            pltpu.make_async_copy(v_in[a], v[a], moment_sem.at[1, a]),
        )

    def fetch(u):
        stage(u).start()
        load(0, u).start()

    first_of_each, rest = order[:2], order[2:]
    for u in first_of_each:
        fetch(u)
    barrier = pltpu.get_barrier_semaphore()
    for other in (partner, ahead, behind):
        pl.semaphore_signal(barrier, inc=1, device_id=other, device_id_type=MESH)
    for u in rest:
        fetch(u)
    for u in first_of_each:
        stage(u).wait()
    pl.semaphore_wait(barrier, 3)
    for u in first_of_each:
        give(0, u, staged=True).start()
    for u in rest:
        stage(u).wait()
        give(0, u, staged=True).start()

    def add(step, u, first=False, squared=None):
        a, layer, start, count = units[u]
        size = m[a].shape[1]
        block = summed(step, u)
        load(step, u).wait()
        give(step, u).wait_recv()
        if not first:
            send_sum(step - 1, u).wait_recv()
        mine, other = (block * CORES + core) * size + start, (block * CORES + 1 - core) * size + start

        def body(i, squared):
            at = pl.ds(pl.multiple_of(mine + i * SLAB, SLAB), SLAB)
            total = whole[a][layer, at, :].astype(jnp.float32)
            total += whole[a][layer, pl.ds(pl.multiple_of(other + i * SLAB, SLAB), SLAB), :].astype(jnp.float32)
            if not first:
                total = slot(step - 1, u)[pl.ds(pl.multiple_of(i * SLAB, SLAB), SLAB), :].astype(jnp.float32) + total
            total = total.astype(jnp.bfloat16)
            whole[a][layer, at, :] = total
            if want is None:
                return 0
            total = total.astype(jnp.float32)
            total = total * total
            pieces = [total[r : r + 8, k : k + 128] for r in range(0, SLAB, 8) for k in range(0, total.shape[1], 128)]
            while len(pieces) > 1:
                pieces = [sum(pieces[k : k + 2]) for k in range(0, len(pieces), 2)]
            return squared + pieces[0]

        want = squared
        return lax.fori_loop(0, count // SLAB, body, 0 if want is None else want)

    def fetch_next(step):
        for u in order:
            load(step + 1, u).start()
            give(step, u).wait_send()
            give(step + 1, u).start()

    for u in order:
        add(0, u, first=True)
        send_sum(0, u).start()
    fetch_next(0)
    for a in range(3):
        for copy in moments(a):
            copy.start()

    def middle(step, carry):
        fetch_next(step)
        for u in order:
            add(step, u)
            send_sum(step - 1, u).wait_send()
            send_sum(step, u).start()
        return carry

    lax.fori_loop(1, chips - 1, middle, 0)
    for u in order:
        own_weights(u).start()

    total = jnp.zeros((8, 128), jnp.float32)
    for u in order:
        total = add(chips - 1, u, squared=total)
    for u in order:
        send_sum(chips - 2, u).wait_send()

    squares[me] = jnp.sum(total, axis=0, keepdims=True)

    free = [ring_send.at[u] for u in order] + [load_sem.at[turn(chips - 1), u] for u in order]

    def norm(k):
        return remote(squares.at[me], squares.at[me], free[k - 1], norm_recv.at[k], {"dp": lax.rem(me + k, n)})

    for k in sorted(range(1, n), key=lambda k: abs(k - n // 2)):
        norm(k).start()
    for u in order:
        give(chips - 1, u).wait_send()
        own_weights(u).wait()
    for a in range(3):
        for copy in moments(a):
            copy.wait()
    for k in range(1, n):
        norm(k).wait()
    every = jnp.sum(jnp.sum(squares[...], axis=0), axis=1, keepdims=True)
    count = n * sum(one.size for one in m)
    factor = jnp.minimum(1.0, 0.5 * lax.rsqrt(every / count + 1e-30))

    for u in order:
        a, layer, first, count = units[u]
        base = me * m[a].shape[1] + first

        def body(i, carry, a=a, layer=layer, u=u, base=base, first=first):
            at = pl.ds(pl.multiple_of(first + i * SLAB, SLAB), SLAB)
            mine = pl.ds(pl.multiple_of(base + i * SLAB, SLAB), SLAB)
            gradient = whole[a][layer, mine, :].astype(jnp.float32) * factor
            weight = w_own(u)[pl.ds(pl.multiple_of(i * SLAB, SLAB), SLAB), :].astype(jnp.float32)
            moment = 0.9 * m[a][layer, at, :] + 0.1 * gradient
            second = 0.95 * v[a][layer, at, :] + 0.05 * gradient * gradient
            m[a][layer, at, :] = moment
            v[a][layer, at, :] = second
            change = moment * lax.rsqrt(second + 1e-8) + 0.1 * weight
            whole[a][layer, mine, :] = (weight - 0.02 * change).astype(jnp.bfloat16)
            return carry

        lax.fori_loop(0, count // SLAB, body, 0)
        send_new(0, u).start()
        pass_new(0, u).start()

    def onward(step, u):
        send_new(step - 1, u).wait()
        pass_new(step - 1, u).wait_send()
        send_new(step, u).start()
        pass_new(step, u).start()

    def later(step, carry):
        for u in order:
            onward(step, u)
        for u in order:
            pass_new(step - 1, u).wait_recv()
        return carry

    lax.fori_loop(1, chips - 1, later, 0)
    for u in order:
        send_new(chips - 2, u).wait()
        pass_new(chips - 2, u).wait_send()
        pass_new(chips - 1, u).start()
    for u in order:
        pass_new(chips - 2, u).wait_recv()
    for u in order:
        pass_new(chips - 1, u).wait()


def write_out(*refs):
    count = (len(refs) - 1) // 2
    copies = []
    for src, dst in zip(refs[:count], refs[count:-1], strict=True):
        parts = PARTS if src.dtype == jnp.bfloat16 else 1
        size = src.shape[1] // parts
        for layer in range(src.shape[0]):
            for part in range(parts):
                at = layer, pl.ds(part * size, size)
                copies.append(pltpu.make_async_copy(src.at[at], dst.at[at], refs[-1].at[len(copies)]))
    for copy in copies:
        copy.start()
    for copy in copies:
        copy.wait()


def solution(mesh):
    n = mesh.shape["dp"]
    chips = n // CORES

    def step(*arrays):
        weights, m, v = (arrays[i : i + 3] for i in (3, 6, 9))
        layers, wide, columns = m[0].shape
        _, tall, narrow = m[2].shape
        unit = layers * PIECES
        whole = [pltpu.VMEM(x.shape, x.dtype) for x in weights]
        states = [pltpu.VMEM(x.shape, x.dtype) for x in (*m, *v)]
        dma = pltpu.SemaphoreType.DMA
        done = pl.pallas_call(
            functools.partial(kernel, n),
            out_shape=[*whole, *states],
            in_specs=[pl.BlockSpec(memory_space=pltpu.HBM)] * 12,
            out_specs=[pl.BlockSpec(memory_space=pltpu.VMEM)] * 9,
            scratch_shapes=[
                pltpu.VMEM((chips - 1, 2 * layers, wide, columns), jnp.bfloat16),
                pltpu.VMEM((chips - 1, layers, tall, narrow), jnp.bfloat16),
                pltpu.VMEM((2 * layers, wide, columns), jnp.bfloat16),
                pltpu.VMEM((layers, tall, narrow), jnp.bfloat16),
                pltpu.VMEM((n, 1, 128), jnp.float32),
                dma((2, unit)),
                dma((unit,)),
                dma((chips, unit)),
                dma((unit,)),
                dma((chips - 1, unit)),
                dma((2, 3)),
                dma((n,)),
            ],
            compiler_params=pltpu.CompilerParams(collective_id=0, has_side_effects=True, vmem_limit_bytes=VMEM_LIMIT),
            name="clipped_step",
        )(*arrays)

        def out(*xs):
            return pl.pallas_call(
                write_out,
                out_shape=[jax.ShapeDtypeStruct(x.shape, x.dtype) for x in xs],
                in_specs=[pl.BlockSpec(memory_space=pltpu.VMEM)] * len(xs),
                out_specs=[pl.BlockSpec(memory_space=pltpu.HBM)] * len(xs),
                scratch_shapes=[dma((sum(layers * (PARTS if x.dtype == jnp.bfloat16 else 1) for x in xs),))],
                compiler_params=pltpu.CompilerParams(vmem_limit_bytes=VMEM_LIMIT),
                name="write_out",
            )(*xs)

        return (*out(*done[:3]), *out(*done[3:]))

    all_of, cut = P(None, None, None), P(None, "dp", None)
    return jax.shard_map(
        step,
        mesh=mesh,
        in_specs=(P(("rep", "dp"), None, None, None),) * 3 + (all_of,) * 3 + (cut,) * 6,
        out_specs=(P("rep", None, None),) * 3 + (P("rep", "dp", None),) * 6,
        check_vma=False,
    )
```
